32 devices in a mesh: seq: 8 (over z, x), head: 4 (over y, core).
Axes of the slice: x: 2, y: 2, z: 4, core: 2. Of those that a mesh axis runs over, the one named last changes fastest.
Arguments:
- queries: bfloat16 [1024, 3072], P('seq', 'head'), may hold values from -8 to 8
- latents: bfloat16 [1024, 576], P('seq'), may hold values from -8 to 8
- key_up: bfloat16 [512, 2048], P(None, 'head'), may hold values from -0.25 to 0.25
- value_up: bfloat16 [512, 2048], P(None, 'head'), may hold values from -0.25 to 0.25
- out_grad: bfloat16 [1024, 2048], P('seq', 'head'), may hold values from -48 to 48
- positions: int32 [1024], P('seq'), may hold values from 0 to 1023, as said below
Outputs:
- query_grad: bfloat16 [1024, 3072], P('seq', 'head')
- latent_grad: float32 [1024, 576], P('seq')
- key_up_grad: float32 [512, 2048], P(None, 'head')
- value_up_grad: float32 [512, 2048], P(None, 'head')
The draws below stay inside these ranges and needn't reach their ends.
Inputs may be any that keep to these rules, and one draw needn't show every extreme that they name: Every position from 0 to 1023 occurs once; positions come in stripes of 128 consecutive positions in ascending order, each stripe whole within the rows of one device.
All inputs are finite; a program needn't handle non-finite values.
Results may differ from the reference program's by a relative error of at most 0.0084.
Values may be sent and summed in bfloat16 or wider, within the bound.
A program may use at most 64 MiB of HBM per device.

```python
import math
import jax
import jax.numpy as jnp
from jax import lax

D_LAT = 512
D_ROPE = 64
D_NOPE = 128
D_V = 128
STRIPE = 128
HEADS = 16
SEQ = 1024


def stripe_positions(key):
    order = jax.random.permutation(jax.random.fold_in(key, 11), SEQ // STRIPE).astype(jnp.int32)
    within = jnp.arange(STRIPE, dtype=jnp.int32)
    return (order[:, None] * STRIPE + within[None, :]).reshape(SEQ)


def draw_positions(key, part):
    return stripe_positions(key)


def draw_queries(key, part):
    width = HEADS * (D_NOPE + D_ROPE)
    own = jax.random.fold_in(key, 21)
    base = jax.random.normal(own, (SEQ, width), jnp.float32)
    return jnp.clip(base, -8.0, 8.0).astype(jnp.bfloat16)


def draw_latents(key, part):
    width = D_LAT + D_ROPE
    own = jax.random.fold_in(key, 31)
    base = jax.random.normal(own, (SEQ, width), jnp.float32)
    return jnp.clip(base, -8.0, 8.0).astype(jnp.bfloat16)


def block_levels(stream_key, extent, pieces, least, top_value):
    factor_of = 1.0
    for position, shards_of in pieces:
        steps = jax.random.uniform(jax.random.fold_in(jax.random.fold_in(stream_key, 6), position), (shards_of,), jnp.float32, least / len(pieces), top_value / len(pieces))
        factor_of = factor_of * jnp.repeat(jnp.exp(steps), extent[position] // shards_of).reshape((-1,) + (1,) * (len(extent) - 1 - position))
    return factor_of


def normal_values(own_key, dims, deviation, limit, pieces=(), held_as=jnp.bfloat16):
    factor_of = block_levels(own_key, dims, pieces, -0.22, 0.18) if pieces else 1.0
    entries = jax.random.normal(own_key, dims, jnp.float32) * deviation * factor_of
    return jnp.minimum(jnp.maximum(entries, -limit), limit).astype(held_as)


def setup_inputs(seed: int = 0) -> dict:
    key_of = jax.random.split(jax.random.key(seed), 7)
    return {
        "queries": draw_queries(jax.random.fold_in(key_of[6], 71), 0),
        "latents": draw_latents(jax.random.fold_in(key_of[6], 71), 0),
        "key_up": normal_values(key_of[2], (D_LAT, HEADS * D_NOPE), D_LAT ** -0.5, 0.25, ((1, 4),)),
        "value_up": normal_values(key_of[3], (D_LAT, HEADS * D_V), D_LAT ** -0.5, 0.25, ((1, 4),)),
        "out_grad": normal_values(key_of[4], (SEQ, HEADS * D_V), 8.0, 48.0, ((0, 8), (1, 4))),
        "positions": draw_positions(jax.random.fold_in(key_of[6], 71), 0),
    }


NEG = -1e+30

def reference(queries, latents, key_up, value_up, out_grad, positions):
    seq = latents.shape[0]
    heads = key_up.shape[1] // D_NOPE
    qk = D_NOPE + D_ROPE
    scale = 1.0 / math.sqrt(qk)
    compressed = latents[:, :D_LAT]
    rope_keys = latents[:, D_LAT:].astype(jnp.float32)
    key_nope = jnp.dot(compressed, key_up, preferred_element_type=jnp.float32).astype(jnp.bfloat16)
    values = jnp.dot(compressed, value_up, preferred_element_type=jnp.float32).astype(jnp.bfloat16)
    key_heads = lax.optimization_barrier(key_nope).astype(jnp.float32).reshape(seq, heads, D_NOPE)
    value_heads = lax.optimization_barrier(values).astype(jnp.float32).reshape(seq, heads, D_V)
    block = math.gcd(seq, 512)
    nblocks = seq // block
    q_blocks = queries.reshape(nblocks, block, heads, qk)
    g_blocks = out_grad.reshape(nblocks, block, heads, D_V)
    p_blocks = positions.reshape(nblocks, block)

    def one_block(carry, inputs):
        key_acc, rope_acc, value_acc = carry
        q_block, g_block, pos_block = inputs
        q_nope = q_block[:, :, :D_NOPE].astype(jnp.float32)
        q_rope = q_block[:, :, D_NOPE:].astype(jnp.float32)
        grads = g_block.astype(jnp.float32)
        scores = jnp.einsum('bhd,khd->hbk', q_nope, key_heads)
        scores = (scores + jnp.einsum('bhd,kd->hbk', q_rope, rope_keys)) * scale
        visible = (positions[None, :] <= pos_block[:, None])[None]
        masked = jnp.where(visible, scores, NEG)
        top = lax.optimization_barrier(jnp.max(masked, axis=2, keepdims=True))
        total = lax.optimization_barrier(jnp.sum(jnp.exp(jnp.where(visible, scores - top, NEG)), axis=2, keepdims=True))
        lse = top + jnp.log(total)
        probs = jnp.exp(jnp.where(visible, scores - lse, NEG))
        dprobs = jnp.einsum('bhd,khd->hbk', grads, value_heads)
        delta = lax.optimization_barrier(jnp.sum(probs * dprobs, axis=2, keepdims=True))
        dscore16 = (probs * (dprobs - delta) * scale).astype(jnp.bfloat16)
        dscore = lax.optimization_barrier(dscore16).astype(jnp.float32)
        probs16 = lax.optimization_barrier(probs.astype(jnp.bfloat16)).astype(jnp.float32)
        grad_nope = jnp.einsum('hbk,khd->bhd', dscore, key_heads)
        grad_rope = jnp.einsum('hbk,kd->bhd', dscore, rope_keys)
        q_grad = jnp.concatenate([grad_nope, grad_rope], axis=2).reshape(block, heads * qk)
        key_acc = key_acc + jnp.einsum('hbk,bhd->khd', dscore, q_nope)
        rope_acc = rope_acc + jnp.einsum('hbk,bhd->kd', dscore, q_rope)
        value_acc = value_acc + jnp.einsum('hbk,bhd->khd', probs16, grads)
        return ((key_acc, rope_acc, value_acc), q_grad.astype(jnp.bfloat16))
    start = (jnp.zeros((seq, heads, D_NOPE), jnp.float32), jnp.zeros((seq, D_ROPE), jnp.float32), jnp.zeros((seq, heads, D_V), jnp.float32))
    sums, q_grads = lax.scan(one_block, start, (q_blocks, g_blocks, p_blocks))
    key_acc, rope_acc, value_acc = sums
    key_grad = key_acc.reshape(seq, heads * D_NOPE)
    value_grad = value_acc.reshape(seq, heads * D_V)
    high = lax.Precision.HIGHEST
    key_up32 = key_up.astype(jnp.float32)
    value_up32 = value_up.astype(jnp.float32)
    folded = jnp.dot(key_grad, key_up32.T, precision=high)
    folded = folded + jnp.dot(value_grad, value_up32.T, precision=high)
    latent_grad = jnp.concatenate([folded, rope_acc], axis=1)
    compressed32 = compressed.astype(jnp.float32)
    key_up_grad = jnp.dot(compressed32.T, key_grad, precision=high)
    value_up_grad = jnp.dot(compressed32.T, value_grad, precision=high)
    query_grad = q_grads.reshape(seq, heads * qk)
    return (query_grad, latent_grad, key_up_grad, value_up_grad)
```

```python
import itertools
import math

import jax
import jax.numpy as jnp
from jax import lax
from jax.experimental import pallas as pl
from jax.experimental.pallas import tpu as pltpu
from jax.sharding import PartitionSpec as P

D_LAT = 512
D_ROPE = 64
D_NOPE = 128
D_V = 128
D_QK = D_NOPE + D_ROPE
LANE = 128
NEG = -1e30
MESH = pl.DeviceIdType.MESH
F32 = jnp.float32
BF16 = jnp.bfloat16


def bit(index, b):
    return (index // (1 << b)) % 2


def flip(index, b):
    return index + (1 << b) * (1 - 2 * bit(index, b))


def with_bits(index, bits, values):
    for b, value in zip(bits, values):
        index = index + (1 << b) * (value - bit(index, b))
    return index


def choices(bits):
    return list(itertools.product((0, 1), repeat=len(bits)))


def nn(a, b):
    return lax.dot_general(a, b, (((1,), (0,)), ((), ())), preferred_element_type=F32)


def nt(a, b):
    return lax.dot_general(a, b, (((1,), (1,)), ((), ())), preferred_element_type=F32)


def tn(a, b):
    return lax.dot_general(a, b, (((0,), (0,)), ((), ())), preferred_element_type=F32)


class Sems:
    def __init__(self, send, recv):
        self.send, self.recv, self.used = send, recv, 0
        self.sent = []

    def copy(self, src, dst, device):
        k = self.used
        self.used += 1
        copy = pltpu.make_async_remote_copy(
            src_ref=src,
            dst_ref=dst,
            send_sem=self.send.at[k],
            recv_sem=self.recv.at[k],
            device_id=device,
            device_id_type=MESH,
        )
        copy.start()
        self.sent.append(copy)
        return copy


def reduce_steps(sems, me, order, device_of, part, slots):
    slot = 0
    for k, b in enumerate(order):
        rest = order[k + 1 :]
        copies = []
        for values in choices(rest):
            leaving = with_bits(flip(me, b), rest, values)
            copies.append((sems.copy(part(leaving), slots.at[slot], device_of(flip(me, b))), slot, values))
            slot += 1
        yield
        for copy, at, values in copies:
            copy.wait_recv()
            kept = part(with_bits(me, rest, values))
            kept[...] = (kept[...].astype(F32) + slots[at].astype(F32)).astype(BF16)


def gather_steps(sems, me, order, device_of, part):
    for k, b in enumerate(order):
        done = order[:k]
        copies = []
        for values in choices(done):
            held = with_bits(me, done, values)
            copies.append(sems.copy(part(held), part(held), device_of(flip(me, b))))
        yield
        for copy in copies:
            copy.wait_recv()


def kernel(
    nseq, nhead,
    q_ref, lat_ref, ku_ref, vu_ref, do_ref, pos_ref,
    dq_ref, dl_ref, dk_ref, dv_ref,
    lat, kk, vv, sc, dp, top, kv, rope, gk, gv, fk, fv, rk, rv, lb, rh, rl, fl, dqs,
    send, recv,
):
    seq, head = lax.axis_index("seq"), lax.axis_index("head")
    seq_bits = list(range(nseq.bit_length() - 1))
    head_bits = list(range(nhead.bit_length() - 1))
    rows = lat_ref.shape[0]
    half = rows // 2
    heads = ku_ref.shape[1] // D_NOPE
    qrows = q_ref.shape[0]
    scale = 1.0 / math.sqrt(D_QK)
    sems = Sems(send, recv)

    def on_seq(s):
        return (s, head)

    def on_head(h):
        return (seq, h)

    barrier = pltpu.get_barrier_semaphore()
    for b in seq_bits:
        pl.semaphore_signal(barrier, inc=1, device_id=on_seq(flip(seq, b)), device_id_type=MESH)
    for b in head_bits:
        pl.semaphore_signal(barrier, inc=1, device_id=on_head(flip(head, b)), device_id_type=MESH)
    pl.semaphore_wait(barrier, len(seq_bits) + len(head_bits))

    core = bit(head, 0)
    other = on_head(flip(head, 0))
    top[...] = jnp.full(top.shape, NEG, F32)

    def mine_of(part):
        return lat.at[pl.ds(pl.multiple_of(part * rows + core * half, half), half)]

    def at_rows(part):
        return pl.ds(pl.multiple_of(part * rows, rows), rows)

    def take(part):
        here = at_rows(part)
        block = lat[here, :]
        comp = block[:, :D_LAT]
        keys = nn(comp, ku_ref[...]).astype(BF16)
        vals = nn(comp, vu_ref[...]).astype(BF16)
        kk[here, :] = keys
        vv[here, :] = vals
        kpos = block[:, D_LAT + D_ROPE :].astype(F32)
        kpos = kpos[:, 0:1] * float(LANE) + kpos[:, 1:2]
        visible = kpos <= pos_ref[...]
        rkeys = block[:, D_LAT : D_LAT + D_ROPE]
        for h in range(heads):
            qn = q_ref[:, h * D_QK : h * D_QK + D_NOPE]
            qr = q_ref[:, h * D_QK + D_NOPE : (h + 1) * D_QK]
            s = nt(keys[:, h * D_NOPE : (h + 1) * D_NOPE], qn) + nt(rkeys, qr)
            s = jnp.where(visible, s * scale, NEG)
            sc[h, here, :] = s
            top[h : h + 1, :] = jnp.maximum(top[h : h + 1, :], jnp.max(s, axis=0, keepdims=True))
            dp[h, here, :] = nt(vals[:, h * D_V : (h + 1) * D_V], do_ref[:, h * D_V : (h + 1) * D_V])

    order = seq_bits[::-1]
    lat[at_rows(seq), :] = lat_ref[...]
    own_half = lat_ref.at[pl.ds(pl.multiple_of(core * half, half), half)]
    fresh = [seq]
    for k, b in enumerate(order):
        copies, parts = [], []
        for values in choices(order[:k]):
            held = with_bits(seq, order[:k], values)
            src = own_half if not any(True for _ in order[:k]) else mine_of(held)
            copies.append(sems.copy(src, mine_of(held), on_seq(flip(seq, b))))
            parts.append(with_bits(flip(seq, b), order[:k], values))
        for part in fresh:
            take(part)
        passed = []
        for copy, part in zip(copies, parts):
            copy.wait_recv()
            passed.append(sems.copy(mine_of(part), mine_of(part), other))
        for copy in passed:
            copy.wait_recv()
        fresh = parts
    for part in fresh:
        take(part)

    tile = math.gcd(lat.shape[0], 256)
    tiles = lat.shape[0] // tile

    def sums(t, carry):
        here = pl.ds(pl.multiple_of(t * tile, tile), tile)
        out = []
        for h in range(heads):
            total, weighted = carry[h]
            p = jnp.exp(sc[h, here, :] - top[h : h + 1, :])
            sc[h, here, :] = p
            total = total + jnp.sum(p, axis=0, keepdims=True)
            weighted = weighted + jnp.sum(p * dp[h, here, :], axis=0, keepdims=True)
            out.append((total, weighted))
        return tuple(out)

    zero = jnp.zeros((1, qrows), F32)
    stats = lax.fori_loop(0, tiles, sums, tuple((zero, zero) for _ in range(heads)))
    inv = [1.0 / total for total, _ in stats]
    delta = [weighted / total for total, weighted in stats]
    dqs[...] = jnp.zeros(dqs.shape, F32)

    def grads(t, carry):
        here = pl.ds(pl.multiple_of(t * tile, tile), tile)
        rkeys = lat[here, D_LAT : D_LAT + D_ROPE]
        rsum = jnp.zeros((tile, D_ROPE), F32)
        for h in range(heads):
            qn = q_ref[:, h * D_QK : h * D_QK + D_NOPE]
            qr = q_ref[:, h * D_QK + D_NOPE : (h + 1) * D_QK]
            prob = sc[h, here, :] * inv[h]
            ds = (prob * (dp[h, here, :] - delta[h]) * scale).astype(BF16)
            kv[here, h * D_NOPE : (h + 1) * D_NOPE] = nn(ds, qn).astype(BF16)
            at = heads * D_NOPE + h * D_V
            kv[here, at : at + D_V] = nn(prob.astype(BF16), do_ref[:, h * D_V : (h + 1) * D_V]).astype(BF16)
            rsum = rsum + nn(ds, qr)
            dqs[h, :, :D_NOPE] += tn(ds, kk[here, h * D_NOPE : (h + 1) * D_NOPE])
            dqs[h, :, D_NOPE:D_QK] += tn(ds, rkeys)
        rope[here, :] = rsum
        return carry

    lax.fori_loop(0, tiles, grads, 0)

    for c in range(D_LAT // LANE):
        up = tn(lat[:, c * LANE : (c + 1) * LANE], kv[...]).astype(BF16)
        gk[c * LANE : (c + 1) * LANE, :] = up[:, : heads * D_NOPE]
        gv[c * LANE : (c + 1) * LANE, :] = up[:, heads * D_NOPE :]

    share = D_LAT // nseq

    def rows_of(ref):
        return lambda part: ref.at[pl.ds(pl.multiple_of(part * share, share), share)]

    def both(source, final, slots, order):
        yield from reduce_steps(sems, seq, order, on_seq, rows_of(source), slots)
        done = rows_of(final)(seq)
        done[...] = rows_of(source)(seq)[...]
        yield from gather_steps(sems, seq, order[::-1], on_seq, rows_of(final))

    def latent_grads():
        sub = rows // nhead

        def fold(part, carry):
            here = at_rows(part)
            total = nt(kv[here, : heads * D_NOPE], ku_ref[...])
            total = total + nt(kv[here, heads * D_NOPE :], vu_ref[...])
            for a in range(nhead):
                cut = slice(a * sub, (a + 1) * sub)
                lb[a, part, :, :D_LAT] = total[cut].astype(BF16)
                lb[a, part, :, D_LAT : D_LAT + D_ROPE] = rope[
                    pl.ds(pl.multiple_of(part * rows + a * sub, sub), sub), :
                ].astype(BF16)
            return carry

        lb[:, :, :, D_LAT:] = jnp.zeros(lb.shape[:3] + (lb.shape[3] - D_LAT,), BF16)
        lax.fori_loop(0, nseq, fold, 0)
        yield from reduce_steps(sems, head, head_bits, on_head, lambda a: lb.at[a], rh)
        mine = lb.at[head]
        yield from reduce_steps(sems, seq, seq_bits, on_seq, lambda s: mine.at[s], rl)
        fl[head] = lb[head, seq]
        yield from gather_steps(sems, head, head_bits[::-1], on_head, lambda a: fl.at[a])

    pipes = [
        both(gv, fv, rv, seq_bits[1:] + seq_bits[:1]),
        both(gk, fk, rk, seq_bits),
        latent_grads(),
    ]
    first = True
    while pipes:
        left = []
        for pipe in pipes:
            try:
                next(pipe)
                left.append(pipe)
            except StopIteration:
                pass
        pipes = left
        if first:
            first = False
            for h in range(heads):
                dq_ref[:, h * D_QK : (h + 1) * D_QK] = dqs[h, :, :D_QK].astype(BF16)
    dk_ref[...] = fk[...].astype(F32)
    dv_ref[...] = fv[...].astype(F32)
    sub = rows // nhead
    for a in range(nhead):
        dl_ref[a * sub : (a + 1) * sub, :] = fl[a, :, : D_LAT + D_ROPE].astype(F32)
    for copy in sems.sent:
        copy.wait_send()


def make_shards(nseq, nhead):
    def shards(queries, latents, key_up, value_up, out_grad, positions):
        rows, heads = latents.shape[0], key_up.shape[1] // D_NOPE
        qrows = queries.shape[0]
        count = rows * nseq
        width = -(-(D_LAT + D_ROPE + 2) // LANE) * LANE
        high, low = positions // LANE, positions % LANE
        coded = jnp.stack([high, low], axis=1).astype(BF16)
        packed = jnp.concatenate(
            [latents, coded, jnp.zeros((rows, width - D_LAT - D_ROPE - 2), BF16)], axis=1
        )
        qpos = positions.astype(F32)[None, :]
        up_cols = heads * D_NOPE
        share = D_LAT // nseq
        sub = rows // nhead
        copies = 6 * (nseq - 1) + (nseq - 1) + 2 * (nhead - 1)
        vmem = pl.BlockSpec(memory_space=pltpu.VMEM)
        body = lambda *refs: kernel(nseq, nhead, *refs)
        return pl.pallas_call(
            body,
            out_shape=(
                jax.ShapeDtypeStruct(queries.shape, BF16),
                jax.ShapeDtypeStruct(latents.shape, F32),
                jax.ShapeDtypeStruct(key_up.shape, F32),
                jax.ShapeDtypeStruct(value_up.shape, F32),
            ),
            in_specs=[vmem] * 6,
            out_specs=(vmem,) * 4,
            scratch_shapes=[
                pltpu.VMEM((count, width), BF16),
                pltpu.VMEM((count, up_cols), BF16),
                pltpu.VMEM((count, up_cols), BF16),
                pltpu.VMEM((heads, count, qrows), F32),
                pltpu.VMEM((heads, count, qrows), F32),
                pltpu.VMEM((heads, qrows), F32),
                pltpu.VMEM((count, 2 * up_cols), BF16),
                pltpu.VMEM((count, D_ROPE), F32),
                pltpu.VMEM((D_LAT, up_cols), BF16),
                pltpu.VMEM((D_LAT, up_cols), BF16),
                pltpu.VMEM((D_LAT, up_cols), BF16),
                pltpu.VMEM((D_LAT, up_cols), BF16),
                pltpu.VMEM((nseq - 1, share, up_cols), BF16),
                pltpu.VMEM((nseq - 1, share, up_cols), BF16),
                pltpu.VMEM((nhead, nseq, sub, width), BF16),
                pltpu.VMEM((nhead - 1, nseq, sub, width), BF16),
                pltpu.VMEM((nseq - 1, sub, width), BF16),
                pltpu.VMEM((nhead, sub, width), BF16),
                pltpu.VMEM((heads, qrows, 2 * LANE), F32),
                pltpu.SemaphoreType.DMA((copies,)),
                pltpu.SemaphoreType.DMA((copies,)),
            ],
            compiler_params=pltpu.CompilerParams(
                collective_id=0, has_side_effects=True, vmem_limit_bytes=60 * 1024 * 1024
            ),
        )(queries, packed, key_up, value_up, out_grad, qpos)

    return shards


def solution(mesh):
    in_specs = (
        P("seq", "head"),
        P("seq", None),
        P(None, "head"),
        P(None, "head"),
        P("seq", "head"),
        P("seq"),
    )
    out_specs = (P("seq", "head"), P("seq", None), P(None, "head"), P(None, "head"))
    shards = make_shards(mesh.shape["seq"], mesh.shape["head"])
    return jax.shard_map(shards, mesh=mesh, in_specs=in_specs, out_specs=out_specs, check_vma=False)
```

```python
import itertools
import math

import jax
import jax.numpy as jnp
from jax import lax
from jax.experimental import pallas as pl
from jax.experimental.pallas import tpu as pltpu
from jax.sharding import PartitionSpec as P

D_LAT = 512
D_ROPE = 64
D_NOPE = 128
D_V = 128
D_QK = D_NOPE + D_ROPE
LANE = 128
NEG = -1e30
MESH = pl.DeviceIdType.MESH
F32 = jnp.float32
BF16 = jnp.bfloat16


def bit(index, b):
    return (index // (1 << b)) % 2


def flip(index, b):
    return index + (1 << b) * (1 - 2 * bit(index, b))


def with_bits(index, bits, values):
    for b, value in zip(bits, values):
        index = index + (1 << b) * (value - bit(index, b))
    return index


def choices(bits):
    return list(itertools.product((0, 1), repeat=len(bits)))


def nn(a, b):
    return lax.dot_general(a, b, (((1,), (0,)), ((), ())), preferred_element_type=F32)


def nt(a, b):
    return lax.dot_general(a, b, (((1,), (1,)), ((), ())), preferred_element_type=F32)


def tn(a, b):
    return lax.dot_general(a, b, (((0,), (0,)), ((), ())), preferred_element_type=F32)


class Sems:
    def __init__(self, send, recv):
        self.send, self.recv, self.used = send, recv, 0
        self.sent = []

    def copy(self, src, dst, device):
        k = self.used
        self.used += 1
        copy = pltpu.make_async_remote_copy(
            src_ref=src,
            dst_ref=dst,
            send_sem=self.send.at[k],
            recv_sem=self.recv.at[k],
            device_id=device,
            device_id_type=MESH,
        )
        copy.start()
        self.sent.append(copy)
        return copy


def reduce_steps(sems, me, order, device_of, part, slots):
    slot = 0
    for k, b in enumerate(order):
        rest = order[k + 1 :]
        copies = []
        for values in choices(rest):
            leaving = with_bits(flip(me, b), rest, values)
            copies.append((sems.copy(part(leaving), slots(slot), device_of(flip(me, b))), slot, values))
            slot += 1
        yield
        for copy, at, values in copies:
            copy.wait_recv()
            kept = part(with_bits(me, rest, values))
            kept[...] = (kept[...].astype(F32) + slots(at)[...].astype(F32)).astype(BF16)


def gather_steps(sems, me, order, device_of, part):
    for k, b in enumerate(order):
        done = order[:k]
        copies = []
        for values in choices(done):
            held = with_bits(me, done, values)
            copies.append(sems.copy(part(held), part(held), device_of(flip(me, b))))
        yield
        for copy in copies:
            copy.wait_recv()


def kernel(
    nseq, nhead,
    q_ref, lat_ref, ku_ref, vu_ref, do_ref, pos_ref,
    dq_ref, dl_ref, dk_ref, dv_ref,
    lat, kk, vv, sc, dp, top, kv, rope, gk, gv, fk, fv, rk, rv, lb, rh, rl, fl, dqs,
    send, recv,
):
    seq, head = lax.axis_index("seq"), lax.axis_index("head")
    seq_bits = list(range(nseq.bit_length() - 1))
    head_bits = list(range(nhead.bit_length() - 1))
    rows = lat_ref.shape[0]
    half = rows // 2
    heads = ku_ref.shape[1] // D_NOPE
    qrows = q_ref.shape[0]
    scale = 1.0 / math.sqrt(D_QK)
    sems = Sems(send, recv)

    def on_seq(s):
        return (s, head)

    def on_head(h):
        return (seq, h)

    barrier = pltpu.get_barrier_semaphore()
    for b in seq_bits:
        pl.semaphore_signal(barrier, inc=1, device_id=on_seq(flip(seq, b)), device_id_type=MESH)
    for b in head_bits:
        pl.semaphore_signal(barrier, inc=1, device_id=on_head(flip(head, b)), device_id_type=MESH)
    pl.semaphore_wait(barrier, len(seq_bits) + len(head_bits))

    core = bit(head, 0)
    other = on_head(flip(head, 0))
    top[...] = jnp.full(top.shape, NEG, F32)

    def at_rows(part):
        return pl.ds(pl.multiple_of(part * rows, rows), rows)

    def take(part):
        here = at_rows(part)
        block = lat[here, :]
        comp = block[:, :D_LAT]
        keys = nn(comp, ku_ref[...]).astype(BF16)
        vals = nn(comp, vu_ref[...]).astype(BF16)
        kk[here, :] = keys
        vv[here, :] = vals
        kpos = block[:, D_LAT + D_ROPE :].astype(F32)
        kpos = kpos[:, 0:1] * float(LANE) + kpos[:, 1:2]
        visible = kpos <= pos_ref[...]
        rkeys = block[:, D_LAT : D_LAT + D_ROPE]
        for h in range(heads):
            qn = q_ref[:, h * D_QK : h * D_QK + D_NOPE]
            qr = q_ref[:, h * D_QK + D_NOPE : (h + 1) * D_QK]
            s = nt(keys[:, h * D_NOPE : (h + 1) * D_NOPE], qn) + nt(rkeys, qr)
            s = jnp.where(visible, s * scale, NEG)
            sc[h, here, :] = s
            top[h : h + 1, :] = jnp.maximum(top[h : h + 1, :], jnp.max(s, axis=0, keepdims=True))
            dp[h, here, :] = nt(vals[:, h * D_V : (h + 1) * D_V], do_ref[:, h * D_V : (h + 1) * D_V])

    piece = half // 2
    down = seq_bits[::-1]
    orders = [down, down[:-2] + down[-2:][::-1]]
    lat[at_rows(seq), :] = lat_ref[...]

    def piece_of(part, p):
        start = part * rows + core * half + p * piece
        return lat.at[pl.ds(pl.multiple_of(start, piece), piece)]

    def bring(p, order):
        own = lat_ref.at[pl.ds(pl.multiple_of(core * half + p * piece, piece), piece)]
        for k, b in enumerate(order):
            copies = []
            for values in choices(order[:k]):
                held = with_bits(seq, order[:k], values)
                src = own if k == 0 else piece_of(held, p)
                part = with_bits(flip(seq, b), order[:k], values)
                copies.append((sems.copy(src, piece_of(held, p), on_seq(flip(seq, b))), part))
            yield None
            passed = []
            for copy, part in copies:
                copy.wait_recv()
                passed.append(sems.copy(piece_of(part, p), piece_of(part, p), other))
            yield passed

    brings = [bring(p, order) for p, order in enumerate(orders)]
    for g in brings:
        next(g)
    common = max(len(down) - 2, 0)
    fresh, waiting = [seq], []
    for k in range(len(down)):
        passed = []
        for g in brings:
            passed += next(g)
            next(g, None)
        for part in fresh:
            take(part)
        fresh = []
        waiting += passed
        if k < common:
            for copy in waiting:
                copy.wait_recv()
            waiting = []
            fresh = [with_bits(flip(seq, down[k]), down[:k], values) for values in choices(down[:k])]
    for part in fresh:
        take(part)
    for copy in waiting:
        copy.wait_recv()
    tail = down[common:]
    for late in choices(tail):
        if not any(late):
            continue
        base = seq
        for b, turned in zip(tail, late):
            base = flip(base, b) if turned else base
        for values in choices(down[:common]):
            take(with_bits(base, down[:common], values))

    tile = math.gcd(lat.shape[0], 256)
    tiles = lat.shape[0] // tile

    def sums(t, carry):
        here = pl.ds(pl.multiple_of(t * tile, tile), tile)
        out = []
        for h in range(heads):
            total, weighted = carry[h]
            p = jnp.exp(sc[h, here, :] - top[h : h + 1, :])
            sc[h, here, :] = p
            total = total + jnp.sum(p, axis=0, keepdims=True)
            weighted = weighted + jnp.sum(p * dp[h, here, :], axis=0, keepdims=True)
            out.append((total, weighted))
        return tuple(out)

    zero = jnp.zeros((1, qrows), F32)
    stats = lax.fori_loop(0, tiles, sums, tuple((zero, zero) for _ in range(heads)))
    inv = [1.0 / total for total, _ in stats]
    delta = [weighted / total for total, weighted in stats]
    dqs[...] = jnp.zeros(dqs.shape, F32)

    def grads(t, carry):
        here = pl.ds(pl.multiple_of(t * tile, tile), tile)
        rkeys = lat[here, D_LAT : D_LAT + D_ROPE]
        rsum = jnp.zeros((tile, D_ROPE), F32)
        for h in range(heads):
            qn = q_ref[:, h * D_QK : h * D_QK + D_NOPE]
            qr = q_ref[:, h * D_QK + D_NOPE : (h + 1) * D_QK]
            prob = sc[h, here, :] * inv[h]
            ds = (prob * (dp[h, here, :] - delta[h]) * scale).astype(BF16)
            kv[here, h * D_NOPE : (h + 1) * D_NOPE] = nn(ds, qn).astype(BF16)
            at = heads * D_NOPE + h * D_V
            kv[here, at : at + D_V] = nn(prob.astype(BF16), do_ref[:, h * D_V : (h + 1) * D_V]).astype(BF16)
            rsum = rsum + nn(ds, qr)
            dqs[h, :, :D_NOPE] += tn(ds, kk[here, h * D_NOPE : (h + 1) * D_NOPE])
            dqs[h, :, D_NOPE:D_QK] += tn(ds, rkeys)
        rope[here, :] = rsum
        return carry

    lax.fori_loop(0, tiles, grads, 0)

    for c in range(D_LAT // LANE):
        up = tn(lat[:, c * LANE : (c + 1) * LANE], kv[...]).astype(BF16)
        gk[c * LANE : (c + 1) * LANE, :] = up[:, : heads * D_NOPE]
        gv[c * LANE : (c + 1) * LANE, :] = up[:, heads * D_NOPE :]

    share = D_LAT // nseq

    half_cols = heads * D_NOPE // 2

    def both(source, final, slots, order, c):
        cols = slice(c * half_cols, (c + 1) * half_cols)

        def rows_of(ref):
            return lambda part: ref.at[pl.ds(pl.multiple_of(part * share, share), share), cols]

        yield from reduce_steps(
            sems, seq, order, on_seq, rows_of(source), lambda k: slots.at[k, :, cols]
        )
        done = rows_of(final)(seq)
        done[...] = rows_of(source)(seq)[...]
        yield from gather_steps(sems, seq, order[::-1], on_seq, rows_of(final))

    def latent_grads():
        sub = rows // nhead

        def fold(part, carry):
            here = at_rows(part)
            total = nt(kv[here, : heads * D_NOPE], ku_ref[...])
            total = total + nt(kv[here, heads * D_NOPE :], vu_ref[...])
            for a in range(nhead):
                cut = slice(a * sub, (a + 1) * sub)
                lb[a, part, :, :D_LAT] = total[cut].astype(BF16)
                lb[a, part, :, D_LAT : D_LAT + D_ROPE] = rope[
                    pl.ds(pl.multiple_of(part * rows + a * sub, sub), sub), :
                ].astype(BF16)
            return carry

        lb[:, :, :, D_LAT:] = jnp.zeros(lb.shape[:3] + (lb.shape[3] - D_LAT,), BF16)
        lax.fori_loop(0, nseq, fold, 0)
        yield from reduce_steps(sems, head, head_bits, on_head, lambda a: lb.at[a], lambda k: rh.at[k])
        mine = lb.at[head]
        yield from reduce_steps(sems, seq, seq_bits, on_seq, lambda s: mine.at[s], lambda k: rl.at[k])
        fl[head] = lb[head, seq]
        yield from gather_steps(sems, head, head_bits[::-1], on_head, lambda a: fl.at[a])

    pipes = [
        both(gv, fv, rv, seq_bits[1:] + seq_bits[:1], 0),
        both(gk, fk, rk, seq_bits, 0),
        both(gv, fv, rv, seq_bits[1:] + seq_bits[:1], 1),
        both(gk, fk, rk, seq_bits, 1),
        latent_grads(),
    ]
    first = True
    while pipes:
        left = []
        for pipe in pipes:
            try:
                next(pipe)
                left.append(pipe)
            except StopIteration:
                pass
        pipes = left
        if first:
            first = False
            for h in range(heads):
                dq_ref[:, h * D_QK : (h + 1) * D_QK] = dqs[h, :, :D_QK].astype(BF16)
    dk_ref[...] = fk[...]
    dv_ref[...] = fv[...]
    sub = rows // nhead
    for a in range(nhead):
        dl_ref[a * sub : (a + 1) * sub, :] = fl[a, :, : D_LAT + D_ROPE]
    for copy in sems.sent:
        copy.wait_send()


def make_shards(nseq, nhead):
    def shards(queries, latents, key_up, value_up, out_grad, positions):
        rows, heads = latents.shape[0], key_up.shape[1] // D_NOPE
        qrows = queries.shape[0]
        count = rows * nseq
        width = -(-(D_LAT + D_ROPE + 2) // LANE) * LANE
        high, low = positions // LANE, positions % LANE
        coded = jnp.stack([high, low], axis=1).astype(BF16)
        packed = jnp.concatenate(
            [latents, coded, jnp.zeros((rows, width - D_LAT - D_ROPE - 2), BF16)], axis=1
        )
        qpos = positions.astype(F32)[None, :]
        up_cols = heads * D_NOPE
        share = D_LAT // nseq
        sub = rows // nhead
        copies = 4 * (nseq - 1) + 8 * (nseq - 1) + (nseq - 1) + 2 * (nhead - 1)
        vmem = pl.BlockSpec(memory_space=pltpu.VMEM)
        body = lambda *refs: kernel(nseq, nhead, *refs)
        dq, dl, dk, dv = pl.pallas_call(
            body,
            out_shape=(
                jax.ShapeDtypeStruct(queries.shape, BF16),
                jax.ShapeDtypeStruct(latents.shape, BF16),
                jax.ShapeDtypeStruct(key_up.shape, BF16),
                jax.ShapeDtypeStruct(value_up.shape, BF16),
            ),
            in_specs=[vmem] * 6,
            out_specs=(vmem,) * 4,
            scratch_shapes=[
                pltpu.VMEM((count, width), BF16),
                pltpu.VMEM((count, up_cols), BF16),
                pltpu.VMEM((count, up_cols), BF16),
                pltpu.VMEM((heads, count, qrows), F32),
                pltpu.VMEM((heads, count, qrows), F32),
                pltpu.VMEM((heads, qrows), F32),
                pltpu.VMEM((count, 2 * up_cols), BF16),
                pltpu.VMEM((count, D_ROPE), F32),
                pltpu.VMEM((D_LAT, up_cols), BF16),
                pltpu.VMEM((D_LAT, up_cols), BF16),
                pltpu.VMEM((D_LAT, up_cols), BF16),
                pltpu.VMEM((D_LAT, up_cols), BF16),
                pltpu.VMEM((nseq - 1, share, up_cols), BF16),
                pltpu.VMEM((nseq - 1, share, up_cols), BF16),
                pltpu.VMEM((nhead, nseq, sub, width), BF16),
                pltpu.VMEM((nhead - 1, nseq, sub, width), BF16),
                pltpu.VMEM((nseq - 1, sub, width), BF16),
                pltpu.VMEM((nhead, sub, width), BF16),
                pltpu.VMEM((heads, qrows, 2 * LANE), F32),
                pltpu.SemaphoreType.DMA((copies,)),
                pltpu.SemaphoreType.DMA((copies,)),
            ],
            compiler_params=pltpu.CompilerParams(
                collective_id=0, has_side_effects=True, vmem_limit_bytes=60 * 1024 * 1024
            ),
        )(queries, packed, key_up, value_up, out_grad, qpos)
        return dq, dl.astype(F32), dk.astype(F32), dv.astype(F32)

    return shards


def solution(mesh):
    in_specs = (
        P("seq", "head"),
        P("seq", None),
        P(None, "head"),
        P(None, "head"),
        P("seq", "head"),
        P("seq"),
    )
    out_specs = (P("seq", "head"), P("seq", None), P(None, "head"), P(None, "head"))
    shards = make_shards(mesh.shape["seq"], mesh.shape["head"])
    return jax.shard_map(shards, mesh=mesh, in_specs=in_specs, out_specs=out_specs, check_vma=False)
```

```python
import itertools
import math

import jax
import jax.numpy as jnp
from jax import lax
from jax.experimental import pallas as pl
from jax.experimental.pallas import tpu as pltpu
from jax.sharding import PartitionSpec as P

D_LAT = 512
D_ROPE = 64
D_NOPE = 128
D_V = 128
D_QK = D_NOPE + D_ROPE
LANE = 128
NEG = -1e30
MESH = pl.DeviceIdType.MESH
F32 = jnp.float32
BF16 = jnp.bfloat16


def bit(index, b):
    return (index // (1 << b)) % 2


def flip(index, b):
    return index + (1 << b) * (1 - 2 * bit(index, b))


def with_bits(index, bits, values):
    for b, value in zip(bits, values):
        index = index + (1 << b) * (value - bit(index, b))
    return index


def choices(bits):
    return list(itertools.product((0, 1), repeat=len(bits)))


def nn(a, b):
    return lax.dot_general(a, b, (((1,), (0,)), ((), ())), preferred_element_type=F32)


def nt(a, b):
    return lax.dot_general(a, b, (((1,), (1,)), ((), ())), preferred_element_type=F32)


def tn(a, b):
    return lax.dot_general(a, b, (((0,), (0,)), ((), ())), preferred_element_type=F32)


class Sems:
    def __init__(self, send, recv):
        self.send, self.recv, self.used = send, recv, 0
        self.sent = []

    def copy(self, src, dst, device):
        k = self.used
        self.used += 1
        copy = pltpu.make_async_remote_copy(
            src_ref=src,
            dst_ref=dst,
            send_sem=self.send.at[k],
            recv_sem=self.recv.at[k],
            device_id=device,
            device_id_type=MESH,
        )
        copy.start()
        self.sent.append(copy)
        return copy


def reduce_steps(sems, me, order, device_of, part, slots):
    slot = 0
    for k, b in enumerate(order):
        rest = order[k + 1 :]
        copies = []
        for values in choices(rest):
            leaving = with_bits(flip(me, b), rest, values)
            copies.append((sems.copy(part(leaving), slots(slot), device_of(flip(me, b))), slot, values))
            slot += 1
        yield
        for copy, at, values in copies:
            copy.wait_recv()
            kept = part(with_bits(me, rest, values))
            kept[...] = (kept[...].astype(F32) + slots(at)[...].astype(F32)).astype(BF16)


def gather_steps(sems, me, order, device_of, part):
    for k, b in enumerate(order):
        done = order[:k]
        copies = []
        for values in choices(done):
            held = with_bits(me, done, values)
            copies.append(sems.copy(part(held), part(held), device_of(flip(me, b))))
        yield
        for copy in copies:
            copy.wait_recv()


def kernel(
    nseq, nhead,
    q_ref, lat_ref, ku_ref, vu_ref, do_ref, pos_ref,
    dq_ref, dl_ref, dk_ref, dv_ref,
    lat, kk, vv, sc, dp, top, kv, rope, gk, gv, fk, fv, rk, rv, lb, rh, rl, fl, dqs,
    send, recv,
):
    seq, head = lax.axis_index("seq"), lax.axis_index("head")
    seq_bits = list(range(nseq.bit_length() - 1))
    head_bits = list(range(nhead.bit_length() - 1))
    rows = lat_ref.shape[0]
    half = rows // 2
    heads = ku_ref.shape[1] // D_NOPE
    qrows = q_ref.shape[0]
    scale = 1.0 / math.sqrt(D_QK)
    sems = Sems(send, recv)

    def on_seq(s):
        return (s, head)

    def on_head(h):
        return (seq, h)

    barrier = pltpu.get_barrier_semaphore()
    for b in seq_bits:
        pl.semaphore_signal(barrier, inc=1, device_id=on_seq(flip(seq, b)), device_id_type=MESH)
    for b in head_bits:
        pl.semaphore_signal(barrier, inc=1, device_id=on_head(flip(head, b)), device_id_type=MESH)
    pl.semaphore_wait(barrier, len(seq_bits) + len(head_bits))

    core = bit(head, 0)
    other = on_head(flip(head, 0))
    top[...] = jnp.full(top.shape, NEG, F32)

    def at_rows(part):
        return pl.ds(pl.multiple_of(part * rows, rows), rows)

    def take(part):
        here = at_rows(part)
        block = lat[here, :]
        comp = block[:, :D_LAT]
        keys = nn(comp, ku_ref[...]).astype(BF16)
        vals = nn(comp, vu_ref[...]).astype(BF16)
        kk[here, :] = keys
        vv[here, :] = vals
        kpos = block[:, D_LAT + D_ROPE :].astype(F32)
        kpos = kpos[:, 0:1] * float(LANE) + kpos[:, 1:2]
        visible = kpos <= pos_ref[...]
        rkeys = block[:, D_LAT : D_LAT + D_ROPE]
        for h in range(heads):
            qn = q_ref[:, h * D_QK : h * D_QK + D_NOPE]
            qr = q_ref[:, h * D_QK + D_NOPE : (h + 1) * D_QK]
            s = nt(keys[:, h * D_NOPE : (h + 1) * D_NOPE], qn) + nt(rkeys, qr)
            s = jnp.where(visible, s * scale, NEG)
            sc[h, here, :] = s
            top[h : h + 1, :] = jnp.maximum(top[h : h + 1, :], jnp.max(s, axis=0, keepdims=True))
            dp[h, here, :] = nt(vals[:, h * D_V : (h + 1) * D_V], do_ref[:, h * D_V : (h + 1) * D_V])

    piece = half // 2
    down = seq_bits[::-1]
    orders = [down, down[:-2] + down[-2:][::-1]]
    lat[at_rows(seq), :] = lat_ref[...]

    def piece_of(part, p):
        start = part * rows + core * half + p * piece
        return lat.at[pl.ds(pl.multiple_of(start, piece), piece)]

    def bring(p, order):
        own = lat_ref.at[pl.ds(pl.multiple_of(core * half + p * piece, piece), piece)]
        for k, b in enumerate(order):
            copies = []
            for values in choices(order[:k]):
                held = with_bits(seq, order[:k], values)
                src = own if k == 0 else piece_of(held, p)
                part = with_bits(flip(seq, b), order[:k], values)
                copies.append((sems.copy(src, piece_of(held, p), on_seq(flip(seq, b))), part))
            yield None
            passed = []
            for copy, part in copies:
                copy.wait_recv()
                passed.append(sems.copy(piece_of(part, p), piece_of(part, p), other))
            yield passed

    brings = [bring(p, order) for p, order in enumerate(orders)]
    for g in brings:
        next(g)
    common = max(len(down) - 2, 0)
    fresh, waiting = [seq], []
    for k in range(len(down)):
        passed = []
        for g in brings:
            passed += next(g)
            next(g, None)
        for part in fresh:
            take(part)
        fresh = []
        waiting += passed
        if k < common:
            for copy in waiting:
                copy.wait_recv()
            waiting = []
            fresh = [with_bits(flip(seq, down[k]), down[:k], values) for values in choices(down[:k])]
    for part in fresh:
        take(part)
    for copy in waiting:
        copy.wait_recv()
    tail = down[common:]
    for late in choices(tail):
        if not any(late):
            continue
        base = seq
        for b, turned in zip(tail, late):
            base = flip(base, b) if turned else base
        for values in choices(down[:common]):
            take(with_bits(base, down[:common], values))

    tile = math.gcd(lat.shape[0], 256)
    tiles = lat.shape[0] // tile

    def sums(t, carry):
        here = pl.ds(pl.multiple_of(t * tile, tile), tile)
        out = []
        for h in range(heads):
            total, weighted = carry[h]
            p = jnp.exp(sc[h, here, :] - top[h : h + 1, :])
            sc[h, here, :] = p
            total = total + jnp.sum(p, axis=0, keepdims=True)
            weighted = weighted + jnp.sum(p * dp[h, here, :], axis=0, keepdims=True)
            out.append((total, weighted))
        return tuple(out)

    zero = jnp.zeros((1, qrows), F32)
    stats = lax.fori_loop(0, tiles, sums, tuple((zero, zero) for _ in range(heads)))
    inv = [1.0 / total for total, _ in stats]
    delta = [weighted / total for total, weighted in stats]
    dqs[...] = jnp.zeros(dqs.shape, F32)

    def grads(t, carry):
        here = pl.ds(pl.multiple_of(t * tile, tile), tile)
        rkeys = lat[here, D_LAT : D_LAT + D_ROPE]
        rsum = jnp.zeros((tile, D_ROPE), F32)
        for h in range(heads):
            qn = q_ref[:, h * D_QK : h * D_QK + D_NOPE]
            qr = q_ref[:, h * D_QK + D_NOPE : (h + 1) * D_QK]
            prob = sc[h, here, :] * inv[h]
            ds = (prob * (dp[h, here, :] - delta[h]) * scale).astype(BF16)
            kv[here, h * D_NOPE : (h + 1) * D_NOPE] = nn(ds, qn).astype(BF16)
            at = heads * D_NOPE + h * D_V
            kv[here, at : at + D_V] = nn(prob.astype(BF16), do_ref[:, h * D_V : (h + 1) * D_V]).astype(BF16)
            rsum = rsum + nn(ds, qr)
            dqs[h, :, :D_NOPE] += tn(ds, kk[here, h * D_NOPE : (h + 1) * D_NOPE])
            dqs[h, :, D_NOPE:D_QK] += tn(ds, rkeys)
        rope[here, :] = rsum
        return carry

    lax.fori_loop(0, tiles, grads, 0)

    for c in range(D_LAT // LANE):
        up = tn(lat[:, c * LANE : (c + 1) * LANE], kv[...]).astype(BF16)
        gk[c * LANE : (c + 1) * LANE, :] = up[:, : heads * D_NOPE]
        gv[c * LANE : (c + 1) * LANE, :] = up[:, heads * D_NOPE :]

    share = D_LAT // nseq

    pieces = heads
    width = heads * D_NOPE // pieces

    def both(source, final, slots, order, c):
        cols = slice(c * width, (c + 1) * width)

        def rows_of(ref):
            return lambda part: ref.at[pl.ds(pl.multiple_of(part * share, share), share), cols]

        yield from reduce_steps(
            sems, seq, order, on_seq, rows_of(source), lambda k: slots.at[k, :, cols]
        )
        done = rows_of(final)(seq)
        done[...] = rows_of(source)(seq)[...]
        yield from gather_steps(sems, seq, order[::-1], on_seq, rows_of(final))

    def latent_grads():
        sub = rows // nhead

        def fold(part, carry):
            here = at_rows(part)
            total = nt(kv[here, : heads * D_NOPE], ku_ref[...])
            total = total + nt(kv[here, heads * D_NOPE :], vu_ref[...])
            for a in range(nhead):
                cut = slice(a * sub, (a + 1) * sub)
                lb[a, part, :, :D_LAT] = total[cut].astype(BF16)
                lb[a, part, :, D_LAT : D_LAT + D_ROPE] = rope[
                    pl.ds(pl.multiple_of(part * rows + a * sub, sub), sub), :
                ].astype(BF16)
            return carry

        lb[:, :, :, D_LAT:] = jnp.zeros(lb.shape[:3] + (lb.shape[3] - D_LAT,), BF16)
        lax.fori_loop(0, nseq, fold, 0)
        yield from reduce_steps(sems, head, head_bits, on_head, lambda a: lb.at[a], lambda k: rh.at[k])
        mine = lb.at[head]
        yield from reduce_steps(sems, seq, seq_bits, on_seq, lambda s: mine.at[s], lambda k: rl.at[k])
        fl[head] = lb[head, seq]
        yield from gather_steps(sems, head, head_bits[::-1], on_head, lambda a: fl.at[a])

    pipes = [
        latent_grads(),
    ]
    for c in reversed(range(pieces)):
        pipes.insert(0, both(gk, fk, rk, seq_bits, c))
        pipes.insert(0, both(gv, fv, rv, seq_bits[1:] + seq_bits[:1], c))
    first = True
    while pipes:
        left = []
        for pipe in pipes:
            try:
                next(pipe)
                left.append(pipe)
            except StopIteration:
                pass
        pipes = left
        if first:
            first = False
            for h in range(heads):
                dq_ref[:, h * D_QK : (h + 1) * D_QK] = dqs[h, :, :D_QK].astype(BF16)
    dk_ref[...] = fk[...]
    dv_ref[...] = fv[...]
    sub = rows // nhead
    for a in range(nhead):
        dl_ref[a * sub : (a + 1) * sub, :] = fl[a, :, : D_LAT + D_ROPE]
    for copy in sems.sent:
        copy.wait_send()


def make_shards(nseq, nhead):
    def shards(queries, latents, key_up, value_up, out_grad, positions):
        rows, heads = latents.shape[0], key_up.shape[1] // D_NOPE
        qrows = queries.shape[0]
        count = rows * nseq
        width = -(-(D_LAT + D_ROPE + 2) // LANE) * LANE
        high, low = positions // LANE, positions % LANE
        coded = jnp.stack([high, low], axis=1).astype(BF16)
        packed = jnp.concatenate(
            [latents, coded, jnp.zeros((rows, width - D_LAT - D_ROPE - 2), BF16)], axis=1
        )
        qpos = positions.astype(F32)[None, :]
        up_cols = heads * D_NOPE
        share = D_LAT // nseq
        sub = rows // nhead
        copies = 4 * (nseq - 1) + 4 * heads * (nseq - 1) + (nseq - 1) + 2 * (nhead - 1)
        vmem = pl.BlockSpec(memory_space=pltpu.VMEM)
        body = lambda *refs: kernel(nseq, nhead, *refs)
        dq, dl, dk, dv = pl.pallas_call(
            body,
            out_shape=(
                jax.ShapeDtypeStruct(queries.shape, BF16),
                jax.ShapeDtypeStruct(latents.shape, BF16),
                jax.ShapeDtypeStruct(key_up.shape, BF16),
                jax.ShapeDtypeStruct(value_up.shape, BF16),
            ),
            in_specs=[vmem] * 6,
            out_specs=(vmem,) * 4,
            scratch_shapes=[
                pltpu.VMEM((count, width), BF16),
                pltpu.VMEM((count, up_cols), BF16),
                pltpu.VMEM((count, up_cols), BF16),
                pltpu.VMEM((heads, count, qrows), F32),
                pltpu.VMEM((heads, count, qrows), F32),
                pltpu.VMEM((heads, qrows), F32),
                pltpu.VMEM((count, 2 * up_cols), BF16),
                pltpu.VMEM((count, D_ROPE), F32),
                pltpu.VMEM((D_LAT, up_cols), BF16),
                pltpu.VMEM((D_LAT, up_cols), BF16),
                pltpu.VMEM((D_LAT, up_cols), BF16),
                pltpu.VMEM((D_LAT, up_cols), BF16),
                pltpu.VMEM((nseq - 1, share, up_cols), BF16),
                pltpu.VMEM((nseq - 1, share, up_cols), BF16),
                pltpu.VMEM((nhead, nseq, sub, width), BF16),
                pltpu.VMEM((nhead - 1, nseq, sub, width), BF16),
                pltpu.VMEM((nseq - 1, sub, width), BF16),
                pltpu.VMEM((nhead, sub, width), BF16),
                pltpu.VMEM((heads, qrows, 2 * LANE), F32),
                pltpu.SemaphoreType.DMA((copies,)),
                pltpu.SemaphoreType.DMA((copies,)),
            ],
            compiler_params=pltpu.CompilerParams(
                collective_id=0, has_side_effects=True, vmem_limit_bytes=60 * 1024 * 1024
            ),
        )(queries, packed, key_up, value_up, out_grad, qpos)
        return dq, dl.astype(F32), dk.astype(F32), dv.astype(F32)

    return shards


def solution(mesh):
    in_specs = (
        P("seq", "head"),
        P("seq", None),
        P(None, "head"),
        P(None, "head"),
        P("seq", "head"),
        P("seq"),
    )
    out_specs = (P("seq", "head"), P("seq", None), P(None, "head"), P(None, "head"))
    shards = make_shards(mesh.shape["seq"], mesh.shape["head"])
    return jax.shard_map(shards, mesh=mesh, in_specs=in_specs, out_specs=out_specs, check_vma=False)
```
